32 devices in a mesh: seq: 16 (over z, y, x), tp: 2 (over core).
Axes of the slice: x: 2, y: 2, z: 4, core: 2. Of those that a mesh axis runs over, the one named last changes fastest.
Arguments:
- inner_input: bfloat16 [4096, 2560], P('seq', 'tp'), may hold values from -6 to 6
- gate_input: bfloat16 [4096, 2560], P('seq', 'tp'), may hold values from -170 to 170
- state_input: bfloat16 [4096, 256], P('seq'), may hold values from -6 to 6
- step_raw: float32 [40, 4096], P('tp', 'seq'), may hold values from -14 to 0
- conv_inner: float32 [4, 2560], P(None, 'tp'), may hold values from -3 to 3
- conv_state: float32 [4, 256], replicated, may hold values from -3 to 3
- bias_inner: float32 [2560], P('tp'), may hold values from -3 to 3
- bias_state: float32 [256], replicated, may hold values from -3 to 3
- step_bias: float32 [40], P('tp'), may hold values from -0.3 to 0.3
- decay_log: float32 [40], P('tp'), may hold values from -1.4 to 0
- skip_gain: float32 [40], P('tp'), may hold values from 0.5 to 1.5
- norm_gain: float32 [2560], P('tp'), may hold values from 0.1 to 1.9
- out_weight: bfloat16 [2560, 2560], P('tp'), may hold values from -0.15625 to 0.15625
Outputs:
- block_out: bfloat16 [4096, 2560], P('seq', 'tp')
The draws below stay inside these ranges and needn't reach their ends.
All inputs are finite; a program needn't handle non-finite values.
Results may differ from the reference program's by a relative error of at most 0.008.
Values may be sent and summed in bfloat16 or wider, within the bound.
No kernel may reach another device: no remote copies, remote signals or barrier semaphores. Data moves between devices by JAX's collectives and lax.ppermute only.
A program may use at most 64 MiB of HBM per device.

```python
import math
import jax
import jax.numpy as jnp
from jax import lax

D = 2560
HEADS = 40
HEAD_DIM = 64
NSTATE = 128
KW = 4
INNER = 2560
TOKEN_COUNT = 4096


def draw_gate_input(key, part):
    second = jax.random.fold_in(key, 1)
    columns = jnp.arange(INNER, dtype=jnp.float32) / INNER
    values = jnp.clip(jax.random.normal(second, (TOKEN_COUNT, INNER)), -5.0, 5.0)
    return (values * jnp.exp(jnp.log(3.0) * columns)[None, :]).astype(jnp.bfloat16)


def draw_step_raw(key, part):
    random_keys = jax.random.split(key, 4)
    share = 0.5
    slow_heads = jax.random.uniform(random_keys[0], (HEADS,)) < share
    base_step = jnp.exp(jax.random.uniform(random_keys[1], (HEADS,), minval=jnp.log(0.05), maxval=jnp.log(0.2)))
    jitter_amount = jnp.exp(jax.random.uniform(random_keys[2], (HEADS, TOKEN_COUNT), minval=-0.7, maxval=0.7))
    spike_points = jax.random.randint(random_keys[3], (4,), 0, TOKEN_COUNT)
    at_spike_point = jnp.any(jnp.arange(TOKEN_COUNT)[None, :] == spike_points[:, None], axis=0)
    gentle_step = jnp.where(at_spike_point[None, :], 0.25, jitter_amount / TOKEN_COUNT)
    target = jnp.where(slow_heads[:, None], gentle_step, base_step[:, None] * jitter_amount)
    return jnp.log(jnp.expm1(target)).astype(jnp.float32)


def with_spikes(result, key, source, target, shards_of, factor):
    owner, partner = [(jnp.arange(result.shape[dim]) // (result.shape[dim] // shards_of)).reshape([-1 if axis == dim else 1 for axis in range(result.ndim)]) for dim in (source, target)]
    chosen = jax.random.permutation(key, shards_of)[partner]
    strong = (owner == chosen) | (owner == (partner + shards_of // 2) % shards_of)
    return jnp.where(strong, factor * result, result)


def block_levels(stream_key, dims, cuts, low, largest):
    loudness, own = 1.0, jax.random.fold_in(stream_key, 6)
    for dim, parts in cuts:
        draws = jnp.exp(jax.random.uniform(jax.random.fold_in(own, dim), (parts,), jnp.float32, low / len(cuts), largest / len(cuts)))
        loudness = loudness * jnp.repeat(draws, dims[dim] // parts).reshape([-1 if axis == dim else 1 for axis in range(len(dims))])
    return loudness


def scatter_about(stream_key, shape, scale, most, shards=(), kind=jnp.bfloat16):
    array = jax.random.normal(stream_key, shape, jnp.float32) * scale
    if len(shards) > 0:
        array = block_levels(stream_key, shape, shards, -0.22, 0.18) * array
    return jnp.clip(array, min=-most, max=most).astype(kind)


def heavy_noise(stream_key, shape, width, most, cuts, heavy, kind=jnp.bfloat16):
    array = width * jax.random.normal(stream_key, shape, jnp.float32)
    if cuts:
        array = array * block_levels(stream_key, shape, cuts, -0.22, 0.18)
    return jnp.clip(with_spikes(array, jax.random.fold_in(stream_key, 3), *heavy), -most, most).astype(kind)


def setup_inputs(seed: int = 0) -> dict:
    seeds = jax.random.split(jax.random.key(seed), 14)
    return {
        "inner_input": scatter_about(seeds[0], (TOKEN_COUNT, INNER), 1.0, 6.0, ((0, 16), (1, 2))),
        "gate_input": draw_gate_input(jax.random.fold_in(seeds[13], 71), 0),
        "state_input": scatter_about(seeds[2], (TOKEN_COUNT, 2 * NSTATE), 1.0, 6.0, ((0, 16),)),
        "step_raw": draw_step_raw(jax.random.fold_in(seeds[13], 71), 0),
        "conv_inner": scatter_about(seeds[4], (KW, INNER), KW ** -0.5, 3.0, ((1, 2),), jnp.float32),
        "conv_state": scatter_about(seeds[5], (KW, 2 * NSTATE), KW ** -0.5, 3.0, (), jnp.float32),
        "bias_inner": scatter_about(seeds[6], (INNER,), 0.5, 3.0, ((0, 2),), jnp.float32),
        "bias_state": scatter_about(seeds[7], (2 * NSTATE,), 0.5, 3.0, (), jnp.float32),
        "step_bias": jnp.clip(jax.random.uniform(seeds[8], (HEADS,), jnp.float32, -0.3, 0.3) * block_levels(seeds[8], (HEADS,), ((0, 2),), -0.4, 0.0), -0.3, 0.3),
        "decay_log": jnp.clip(-1.4 + 1.4 * jax.random.uniform(seeds[9], (HEADS,), jnp.float32) ** block_levels(seeds[9], (HEADS,), ((0, 2),), -0.2, 0.2), -1.4, 0.0),
        "skip_gain": jnp.clip(0.5 + 1.0 * jax.random.uniform(seeds[10], (HEADS,), jnp.float32) ** block_levels(seeds[10], (HEADS,), ((0, 2),), -0.2, 0.2), 0.5, 1.5),
        "norm_gain": jnp.clip(1.0 + 0.18 * jax.random.normal(seeds[11], (INNER,), jnp.float32), 0.1, 1.9),
        "out_weight": heavy_noise(seeds[12], (INNER, D), INNER ** -0.5, 0.15625, ((0, 2),), (0, 1, 2, 2.0)),
    }


highest = lax.Precision.HIGHEST

def conv_silu(padded, weights, offsets, length):
    width_taps = weights.shape[0]
    summed = offsets.astype(jnp.float32)[None, :] + jnp.zeros((length, weights.shape[1]), jnp.float32)
    for number in range(width_taps):
        summed = summed + weights[number][None, :] * padded[number:number + length]
    return jax.nn.silu(summed).astype(jnp.bfloat16)

def block_step(state_now, pieces):
    inner_rows, keys_b, query_c, step_sizes, log_decay = pieces
    cumulative = jnp.cumsum(log_decay, axis=1)
    block_rows = log_decay.shape[1]
    causal = jnp.arange(block_rows)[:, None] >= jnp.arange(block_rows)[None, :]
    spread = jnp.where(causal[None], cumulative[:, :, None] - cumulative[:, None, :], -jnp.inf)
    scores = jnp.dot(query_c, keys_b.T, precision=highest)
    weights = scores[None] * jnp.exp(spread) * step_sizes[:, None, :]
    output = jnp.einsum('hts,shp->thp', weights, inner_rows, precision=highest)
    carried = jnp.einsum('tn,hnp->thp', query_c, state_now, precision=highest)
    output = output + carried * jnp.exp(cumulative).T[:, :, None]
    towards_end = jnp.exp(cumulative[:, -1:] - cumulative) * step_sizes
    update = jnp.einsum('sn,shp->hnp', keys_b, inner_rows * towards_end.T[:, :, None], precision=highest)
    state_next = jnp.exp(cumulative[:, -1])[:, None, None] * state_now + update
    return (state_next, output)

def reference(inner_input, gate_input, state_input, step_raw, conv_inner, conv_state, bias_inner, bias_state, step_bias, decay_log, skip_gain, norm_gain, out_weight):
    width_taps = conv_inner.shape[0]
    pad_rows = ((width_taps - 1, 0), (0, 0))
    inner_conv = conv_silu(jnp.pad(inner_input.astype(jnp.float32), pad_rows), conv_inner, bias_inner, TOKEN_COUNT)
    state_conv = conv_silu(jnp.pad(state_input.astype(jnp.float32), pad_rows), conv_state, bias_state, TOKEN_COUNT)
    step_sizes = jax.nn.softplus(step_raw + step_bias[:, None])
    log_decay = -jnp.exp(decay_log)[:, None] * step_sizes
    block_size = math.gcd(TOKEN_COUNT, 256)
    blocks = TOKEN_COUNT // block_size
    inner_float = inner_conv.astype(jnp.float32)
    inner_rows = inner_float.reshape(blocks, block_size, HEADS, HEAD_DIM)
    keys_b = state_conv[:, :NSTATE].astype(jnp.float32).reshape(blocks, block_size, NSTATE)
    query_c = state_conv[:, NSTATE:].astype(jnp.float32).reshape(blocks, block_size, NSTATE)
    step_block_grid = step_sizes.reshape(HEADS, blocks, block_size).transpose(1, 0, 2)
    log_blocks = log_decay.reshape(HEADS, blocks, block_size).transpose(1, 0, 2)
    start_state = jnp.zeros((HEADS, NSTATE, HEAD_DIM), jnp.float32)
    final_state, outputs = lax.scan(block_step, start_state, (inner_rows, keys_b, query_c, step_block_grid, log_blocks))
    mixed = outputs.reshape(TOKEN_COUNT, HEADS, HEAD_DIM) + skip_gain[None, :, None] * inner_float.reshape(TOKEN_COUNT, HEADS, HEAD_DIM)
    gated_raw = mixed.reshape(TOKEN_COUNT, INNER) * jax.nn.silu(gate_input.astype(jnp.float32))
    squares = lax.optimization_barrier(jnp.sum(gated_raw * gated_raw, axis=1))
    scale_inv = lax.rsqrt(squares / INNER + 1e-05)
    gated = (gated_raw * norm_gain[None, :]).astype(jnp.bfloat16)
    summed = jnp.dot(gated, out_weight, preferred_element_type=jnp.float32)
    return (summed * scale_inv[:, None]).astype(jnp.bfloat16)
```

```python
import functools
import jax
import jax.numpy as jnp
from jax import lax
from jax.experimental import pallas as pl
from jax.experimental.pallas import tpu as pltpu
from jax.sharding import PartitionSpec as P

HEAD_DIM = 64
SPREAD = 64
LANES = 128
LOG2E = 1.4426950408889634
highest = lax.Precision.HIGHEST
f32 = jnp.float32
bf16 = jnp.bfloat16


def dot(a, b, contract, precision=None):
    return lax.dot_general(
        a, b, (contract, ((), ())), precision=precision, preferred_element_type=f32
    )


def silu(v):
    return v / (1.0 + jnp.exp(-v))


def spread_matrix(width):
    rows = lax.broadcasted_iota(jnp.int32, (2 * SPREAD, width), 0) & (SPREAD - 1)
    heads = lax.broadcasted_iota(jnp.int32, (2 * SPREAD, width), 1) >> (HEAD_DIM.bit_length() - 1)
    return jnp.where(rows == heads, 1.0, 0.0).astype(bf16)


def split_rows(ref, value):
    heads = value.shape[0]
    high = value.astype(bf16).astype(f32)
    ref[...] = jnp.zeros_like(ref)
    ref[0:heads, :] = high
    ref[SPREAD : SPREAD + heads, :] = value - high
    return ref[...].astype(bf16)


def steps(raw_ref, step_bias_ref, decay_ref):
    v = raw_ref[...] + step_bias_ref[...]
    x = jnp.exp(-jnp.abs(v))
    series = x * (1.0 - x * (0.5 - x * (1.0 / 3.0 - x * 0.25)))
    size = jnp.maximum(v, 0.0) + jnp.where(x < 0.01, series, jnp.log(1.0 + x))
    return size, -jnp.exp(decay_ref[...]) * size


def lower(rows):
    t = lax.broadcasted_iota(jnp.int32, (rows, rows), 0)
    s = lax.broadcasted_iota(jnp.int32, (rows, rows), 1)
    return jnp.where(t >= s, 1.0, 0.0).astype(f32)


def conv_block(scratch, taps_ref, bias_ref, cols, rows):
    taps = taps_ref.shape[0]
    first = 8 - (taps - 1)
    total = jnp.broadcast_to(bias_ref[:, cols], (rows, bias_ref[:, cols].shape[1]))
    for number in range(taps):
        total = total + taps_ref[number : number + 1, cols] * scratch[
            pl.ds(first + number, rows), cols
        ]
    return silu(total)


def update_kernel(
    inner_ref, state_ref, halo_ref, raw_ref, step_bias_ref, decay_ref,
    taps_ref, bias_ref, state_taps_ref, state_bias_ref,
    x_ref, bc_ref, payload_ref, pad, state_pad, parts,
):
    rows, width = inner_ref.shape
    states = state_ref.shape[1]
    half = states // 2
    state_pad[0:8, :] = halo_ref[:, width:].astype(f32)
    state_pad[8:, :] = state_ref[...].astype(f32)
    bc_ref[...] = conv_block(state_pad, state_taps_ref, state_bias_ref, slice(0, states), rows).astype(bf16)
    keys = bc_ref[:, :half]
    size, decay = steps(raw_ref, step_bias_ref, decay_ref)
    cum = dot(decay, lower(rows), ((1,), (1,)), highest)
    weight = jnp.exp(cum[:, rows - 1 :] - cum) * size
    weight = split_rows(parts, weight)
    spread = spread_matrix(width)
    pad[0:8, :] = halo_ref[:, :width].astype(f32)
    pad[8:, :] = inner_ref[...].astype(f32)
    block = 256
    for start in range(0, width, block):
        cols = slice(start, start + block)
        value = conv_block(pad, taps_ref, bias_ref, cols, rows).astype(bf16)
        x_ref[:, cols] = value
        scale = dot(weight, spread[:, cols], ((0,), (0,)))
        scaled = (value.astype(f32) * scale).astype(bf16)
        payload_ref[:, cols] = dot(keys, scaled, ((0,), (0,))).astype(bf16)
    heads = raw_ref.shape[0]
    total = jnp.exp(dot(jnp.ones((half, rows), f32), decay, ((1,), (1,)), highest))
    high = total.astype(bf16)
    payload_ref[:, width:] = jnp.zeros((half, LANES), bf16)
    payload_ref[:, width : width + heads] = high
    payload_ref[:, width + SPREAD : width + SPREAD + heads] = (total - high.astype(f32)).astype(bf16)


def inside_kernel(x_ref, bc_ref, raw_ref, step_bias_ref, decay_ref, skip_ref, y_ref):
    rows = x_ref.shape[0]
    half = bc_ref.shape[1] // 2
    heads = raw_ref.shape[0]
    size, decay = steps(raw_ref, step_bias_ref, decay_ref)
    tri = lower(rows)
    cum = dot(decay, tri, ((1,), (1,)), highest) * LOG2E
    col = dot(tri, decay, ((1,), (1,)), highest) * LOG2E
    row = cum - jnp.log(size) * LOG2E
    mid = rows // 2
    scores = dot(bc_ref[:, half:], bc_ref[:, :half], ((1,), (1,)))
    causal = tri[:mid, :mid] > 0.5
    top = jnp.where(causal, scores[:mid, :mid], 0.0)
    low_left = scores[mid:, :mid]
    low_right = jnp.where(causal, scores[mid:, mid:], 0.0)
    for h in range(heads):
        cols = slice(h * HEAD_DIM, (h + 1) * HEAD_DIM)
        x = x_ref[:, cols]
        c0, c1 = col[:mid, h : h + 1], col[mid:, h : h + 1]
        r0, r1 = row[h : h + 1, :mid], row[h : h + 1, mid:]
        w0 = (top * jnp.exp2(jnp.minimum(c0 - r0, 100.0))).astype(bf16)
        w1 = (low_left * jnp.exp2(c1 - r0)).astype(bf16)
        w2 = (low_right * jnp.exp2(jnp.minimum(c1 - r1, 100.0))).astype(bf16)
        gain = skip_ref[h, 0]
        y_ref[:mid, cols] = dot(w0, x[:mid], ((1,), (0,))) + gain * x[:mid].astype(f32)
        y_ref[mid:, cols] = (
            dot(w1, x[:mid], ((1,), (0,))) + dot(w2, x[mid:], ((1,), (0,)))
            + gain * x[mid:].astype(f32)
        )


def prefix_kernel(devices, got_ref, out_ref):
    width = out_ref.shape[1]
    each = got_ref.shape[0] // devices
    spread = spread_matrix(width)
    decays = dot(got_ref[:, width:], spread, ((1,), (0,)))
    update = got_ref[:, :width].astype(f32)
    running = jnp.zeros((each, width), f32)
    found = []
    for d in range(devices):
        found.append(running)
        rows = slice(d * each, (d + 1) * each)
        if d < devices - 1:
            running = running * decays[rows] + update[rows]
    out_ref[...] = jnp.concatenate(found, axis=0).astype(bf16)


def gate_kernel(
    me_ref, entering_ref, bc_ref, y_ref, raw_ref, step_bias_ref, decay_ref,
    gate_ref, gain_ref, weight_ref, gated_ref, squares_ref, send_ref, parts,
):
    rows, width = y_ref.shape
    half = bc_ref.shape[1] // 2
    _, decay = steps(raw_ref, step_bias_ref, decay_ref)
    cum = jnp.exp(dot(decay, lower(rows), ((1,), (1,)), highest))
    factor = split_rows(parts, cum)
    spread = spread_matrix(width)
    query = bc_ref[:, half:]
    squares = jnp.zeros((rows, LANES), f32)
    block = 256
    for start in range(0, width, block):
        cols = slice(start, start + block)
        carried = dot(query, entering_ref[:, cols], ((1,), (0,)))
        scale = dot(factor, spread[:, cols], ((0,), (0,)))
        mixed = y_ref[:, cols] + carried * scale
        raw = mixed * silu(gate_ref[:, cols].astype(f32))
        for lane in range(0, block, LANES):
            piece = raw[:, lane : lane + LANES]
            squares = squares + piece * piece
        gated_ref[:, cols] = (raw * gain_ref[:, cols]).astype(bf16)
    total = jnp.sum(squares, axis=1, keepdims=True)
    squares_ref[...] = jnp.broadcast_to(total, (rows, LANES))
    high = total.astype(bf16)
    low = (total - high.astype(f32)).astype(bf16)
    lane = lax.broadcasted_iota(jnp.int32, (rows, LANES), 1)
    send_ref[:, width:] = jnp.where(
        lane < SPREAD,
        jnp.broadcast_to(high.astype(f32), (rows, LANES)),
        jnp.broadcast_to(low.astype(f32), (rows, LANES)),
    ).astype(bf16)
    peer = pl.multiple_of((1 - me_ref[0, 0]) * width, LANES)
    send_ref[:, :width] = dot(
        gated_ref[...], weight_ref[:, pl.ds(peer, width)], ((1,), (0,))
    ).astype(bf16)


def own_kernel(me_ref, gated_ref, weight_ref, own_ref):
    width = gated_ref.shape[1]
    mine = pl.multiple_of(me_ref[0, 0] * width, LANES)
    own_ref[...] = dot(gated_ref[...], weight_ref[:, pl.ds(mine, width)], ((1,), (0,)))


def finish_kernel(inner, own_ref, squares_ref, got_ref, out_ref):
    width = own_ref.shape[1]
    other = got_ref[:, width:].astype(f32)
    total = squares_ref[:, :1] + other[:, :1] + other[:, SPREAD : SPREAD + 1]
    scale = lax.rsqrt(total / inner + 1e-05)
    out_ref[...] = ((own_ref[...] + got_ref[:, :width].astype(f32)) * scale).astype(bf16)


VMEM = pl.BlockSpec(memory_space=pltpu.VMEM)
SMEM = pl.BlockSpec(memory_space=pltpu.SMEM)


def call(kernel, specs, outs, flops, scratch=(), limit=40):
    one = not isinstance(outs, (list, tuple))
    return pl.pallas_call(
        kernel,
        out_shape=outs,
        in_specs=specs,
        out_specs=VMEM if one else [VMEM] * len(outs),
        scratch_shapes=list(scratch),
        compiler_params=pltpu.CompilerParams(vmem_limit_bytes=limit << 20),
        cost_estimate=pl.CostEstimate(flops=int(flops), bytes_accessed=1 << 20, transcendentals=0),
    )


def local(
    inner_input, gate_input, state_input, step_raw, conv_inner, conv_state,
    bias_inner, bias_state, step_bias, decay_log, skip_gain, norm_gain, out_weight,
):
    rows, width = inner_input.shape
    heads = step_raw.shape[0]
    states = state_input.shape[1]
    half = states // 2
    devices = lax.axis_size("seq")
    halo = lax.ppermute(
        jnp.concatenate([inner_input[rows - 8 :], state_input[rows - 8 :]], axis=1),
        "seq",
        [(d, d + 1) for d in range(devices - 1)],
    )
    step_args = (step_raw, step_bias[:, None], decay_log[:, None])
    shape = jax.ShapeDtypeStruct
    x, bc, payload = call(
        update_kernel,
        [VMEM] * 10,
        [shape((rows, width), bf16), shape((rows, states), bf16), shape((half, width + LANES), bf16)],
        2e9,
        [
            pltpu.VMEM((rows + 8, width), f32),
            pltpu.VMEM((rows + 8, states), f32),
            pltpu.VMEM((2 * SPREAD, rows), f32),
        ],
    )(
        inner_input, state_input, halo, *step_args,
        conv_inner, bias_inner[None], conv_state, bias_state[None],
    )
    each = half // devices
    got = lax.all_to_all(
        payload.reshape(devices, each, width + LANES), "seq", split_axis=0, concat_axis=0, tiled=True
    )
    y = call(inside_kernel, [VMEM] * 5 + [SMEM], shape((rows, width), f32), 4e9)(
        x, bc, *step_args, skip_gain[:, None]
    )
    before = call(
        functools.partial(prefix_kernel, devices), [VMEM], shape((half, width), bf16), 1e8
    )(got.reshape(half, width + LANES))
    entering = lax.all_to_all(
        before.reshape(devices, each, width), "seq", split_axis=0, concat_axis=0, tiled=True
    ).reshape(half, width)
    me = lax.axis_index("tp").astype(jnp.int32).reshape(1, 1)
    gated, squares, send = call(
        gate_kernel,
        [SMEM] + [VMEM] * 9,
        [shape((rows, width), bf16), shape((rows, LANES), f32), shape((rows, width + LANES), bf16)],
        2e9,
        [pltpu.VMEM((2 * SPREAD, rows), f32)],
    )(me, entering, bc, y, *step_args, gate_input, norm_gain[None], out_weight)
    pairs = lax.axis_size("tp")
    other = lax.ppermute(send, "tp", [(d, pairs - 1 - d) for d in range(pairs)])
    own = call(own_kernel, [SMEM, VMEM, VMEM], shape((rows, width), f32), 2e9)(
        me, gated, out_weight
    )
    return call(
        functools.partial(finish_kernel, float(width * pairs)),
        [VMEM] * 3, shape((rows, width), bf16), 1e8,
    )(own, squares, other)


def solution(mesh):
    return jax.shard_map(
        local,
        mesh=mesh,
        in_specs=(
            P("seq", "tp"), P("seq", "tp"), P("seq", None), P("tp", "seq"), P(None, "tp"), P(),
            P("tp"), P(), P("tp"), P("tp"), P("tp"), P("tp"), P("tp", None),
        ),
        out_specs=P("seq", "tp"),
        check_vma=False,
    )
```

```python
import functools
import jax
import jax.numpy as jnp
from jax import lax
from jax.experimental import pallas as pl
from jax.experimental.pallas import tpu as pltpu
from jax.sharding import PartitionSpec as P

HEAD_DIM = 64
SPREAD = 64
LANES = 128
LOG2E = 1.4426950408889634
highest = lax.Precision.HIGHEST
f32 = jnp.float32
bf16 = jnp.bfloat16


def dot(a, b, contract, precision=None):
    return lax.dot_general(
        a, b, (contract, ((), ())), precision=precision, preferred_element_type=f32
    )


def silu(v):
    return v / (1.0 + jnp.exp(-v))


def spread_matrix(width):
    rows = lax.broadcasted_iota(jnp.int32, (2 * SPREAD, width), 0) & (SPREAD - 1)
    heads = lax.broadcasted_iota(jnp.int32, (2 * SPREAD, width), 1) >> (HEAD_DIM.bit_length() - 1)
    return jnp.where(rows == heads, 1.0, 0.0).astype(bf16)


def split_rows(ref, value):
    heads = value.shape[0]
    high = value.astype(bf16).astype(f32)
    ref[...] = jnp.zeros_like(ref)
    ref[0:heads, :] = high
    ref[SPREAD : SPREAD + heads, :] = value - high
    return ref[...].T.astype(bf16)


def as_column(row):
    count = row.shape[1]
    a = lax.broadcasted_iota(jnp.int32, (count, count), 0)
    b = lax.broadcasted_iota(jnp.int32, (count, count), 1)
    return jnp.sum(jnp.where(a == b, jnp.broadcast_to(row, (count, count)), 0.0), axis=1, keepdims=True)


def steps(raw_ref, step_bias_ref, decay_ref):
    v = raw_ref[...] + as_column(step_bias_ref[...])
    x = jnp.exp(-jnp.abs(v))
    series = x * (1.0 - x * (0.5 - x * (1.0 / 3.0 - x * 0.25)))
    size = jnp.maximum(v, 0.0) + jnp.where(x < 0.01, series, jnp.log(1.0 + x))
    return size, -jnp.exp(as_column(decay_ref[...])) * size


def lower(rows):
    t = lax.broadcasted_iota(jnp.int32, (rows, rows), 0)
    s = lax.broadcasted_iota(jnp.int32, (rows, rows), 1)
    return jnp.where(t >= s, 1.0, 0.0).astype(f32)


def row_of(ref, cols):
    first, last = cols.start // LANES, cols.stop // LANES
    return jnp.concatenate([ref[r : r + 1, :] for r in range(first, last)], axis=1)


def conv_block(scratch, taps_ref, bias_ref, cols, rows):
    taps = taps_ref.shape[0]
    first = 8 - (taps - 1)
    total = jnp.broadcast_to(row_of(bias_ref, cols), (rows, cols.stop - cols.start))
    for number in range(taps):
        total = total + taps_ref[number : number + 1, cols] * scratch[
            pl.ds(first + number, rows), cols
        ]
    return silu(total)


def update_kernel(count, *refs):
    sources, (x_out, bc_out, payload_out) = refs[:count], refs[count : count + 3]
    kept, rest = refs[count + 3 : 2 * count + 3], refs[2 * count + 3 :]
    (
        halo_ref, raw_ref, step_bias_ref, decay_ref, state_taps_ref, state_bias_ref, state_ref,
        taps_ref, bias_ref, inner_ref,
    ) = kept
    x_ref, bc_ref, payload_ref, pad, state_pad, parts, in_sems, out_sems = rest
    copies = [
        pltpu.make_async_copy(a, b, in_sems.at[i]) for i, (a, b) in enumerate(zip(sources, kept))
    ]
    for copy in copies:
        copy.start()
    for copy in copies[:-1]:
        copy.wait()
    rows, width = inner_ref.shape
    leaving = []

    def leave(source, target):
        copy = pltpu.make_async_copy(source, target, out_sems.at[len(leaving)])
        copy.start()
        leaving.append(copy)

    states = state_ref.shape[1]
    half = states // 2
    state_pad[0:8, :] = halo_ref[:, width:].astype(f32)
    state_pad[8:, :] = state_ref[...].astype(f32)
    bc_ref[...] = conv_block(state_pad, state_taps_ref, state_bias_ref, slice(0, states), rows).astype(bf16)
    leave(bc_ref, bc_out)
    keys = bc_ref[:, :half].astype(f32).T.astype(bf16)
    size, decay = steps(raw_ref, step_bias_ref, decay_ref)
    heads = raw_ref.shape[0]
    parts[...] = jnp.zeros_like(parts)
    parts[0:heads, :] = decay
    parts[SPREAD : SPREAD + heads, :] = decay
    total = jnp.exp(dot(jnp.ones((half, rows), f32), parts[...], ((1,), (1,)), highest))
    high = total.astype(bf16).astype(f32)
    lane = lax.broadcasted_iota(jnp.int32, (half, LANES), 1)
    payload_ref[:, width:] = jnp.where(lane < SPREAD, high, total - high).astype(bf16)
    cum = dot(decay, lower(rows), ((1,), (1,)), highest)
    weight = jnp.exp(cum[:, rows - 1 :] - cum) * size
    weight = split_rows(parts, weight)
    spread = spread_matrix(width)
    copies[-1].wait()
    pad[0:8, :] = halo_ref[:, :width].astype(f32)
    pad[8:, :] = inner_ref[...].astype(f32)
    last = slice(width, width + LANES)
    leave(payload_ref.at[:, last], payload_out.at[:, last])
    block = 256
    for start in range(0, width, block):
        cols = slice(start, start + block)
        value = conv_block(pad, taps_ref, bias_ref, cols, rows).astype(bf16)
        x_ref[:, cols] = value
        leave(x_ref.at[:, cols], x_out.at[:, cols])
        scale = dot(weight, spread[:, cols], ((1,), (0,)))
        scaled = (value.astype(f32) * scale).astype(bf16)
        payload_ref[:, cols] = dot(keys, scaled, ((1,), (0,))).astype(bf16)
        leave(payload_ref.at[:, cols], payload_out.at[:, cols])
    for copy in leaving:
        copy.wait()


def inside_kernel(x_ref, bc_ref, raw_ref, step_bias_ref, decay_ref, skip_ref, y_ref):
    rows = x_ref.shape[0]
    half = bc_ref.shape[1] // 2
    heads = raw_ref.shape[0]
    size, decay = steps(raw_ref, step_bias_ref, decay_ref)
    tri = lower(rows)
    cum = dot(decay, tri, ((1,), (1,)), highest) * LOG2E
    col = dot(tri, decay, ((1,), (1,)), highest) * LOG2E
    row = cum - jnp.log(size) * LOG2E
    mid = rows // 2
    scores = dot(bc_ref[:, half:], bc_ref[:, :half], ((1,), (1,)))
    causal = tri[:mid, :mid] > 0.5
    top = jnp.where(causal, scores[:mid, :mid], 0.0)
    low_left = scores[mid:, :mid]
    low_right = jnp.where(causal, scores[mid:, mid:], 0.0)
    for h in range(heads):
        cols = slice(h * HEAD_DIM, (h + 1) * HEAD_DIM)
        x = x_ref[:, cols]
        c0, c1 = col[:mid, h : h + 1], col[mid:, h : h + 1]
        r0, r1 = row[h : h + 1, :mid], row[h : h + 1, mid:]
        w0 = (top * jnp.exp2(jnp.minimum(c0 - r0, 100.0))).astype(bf16)
        w1 = (low_left * jnp.exp2(c1 - r0)).astype(bf16)
        w2 = (low_right * jnp.exp2(jnp.minimum(c1 - r1, 100.0))).astype(bf16)
        gain = skip_ref[h]
        y_ref[:mid, cols] = dot(w0, x[:mid], ((1,), (0,))) + gain * x[:mid].astype(f32)
        y_ref[mid:, cols] = (
            dot(w1, x[:mid], ((1,), (0,))) + dot(w2, x[mid:], ((1,), (0,)))
            + gain * x[mid:].astype(f32)
        )


def prefix_kernel(devices, got_ref, out_ref):
    width = out_ref.shape[1]
    each = got_ref.shape[0] // devices
    spread = spread_matrix(width)
    decays = dot(got_ref[:, width:], spread, ((1,), (0,)))
    update = got_ref[:, :width].astype(f32)
    running = jnp.zeros((each, width), f32)
    found = []
    for d in range(devices):
        found.append(running)
        rows = slice(d * each, (d + 1) * each)
        if d < devices - 1:
            running = running * decays[rows] + update[rows]
    out_ref[...] = jnp.concatenate(found, axis=0).astype(bf16)


def gate_kernel(
    me_ref, entering_ref, bc_ref, y_ref, raw_ref, step_bias_ref, decay_ref,
    gate_ref, gain_ref, weight_ref, gated_ref, squares_ref, send_ref, mine_ref,
    parts, theirs_ref, sems,
):
    rows, width = y_ref.shape
    me = me_ref[0, 0]
    peer = pl.multiple_of((1 - me) * width, LANES)
    mine = pl.multiple_of(me * width, LANES)
    first = pltpu.make_async_copy(weight_ref.at[:, pl.ds(peer, width)], theirs_ref, sems.at[0])
    second = pltpu.make_async_copy(weight_ref.at[:, pl.ds(mine, width)], mine_ref, sems.at[1])
    first.start()
    second.start()
    half = bc_ref.shape[1] // 2
    _, decay = steps(raw_ref, step_bias_ref, decay_ref)
    cum = jnp.exp(dot(decay, lower(rows), ((1,), (1,)), highest))
    factor = split_rows(parts, cum)
    spread = spread_matrix(width)
    query = bc_ref[:, half:]
    squares = jnp.zeros((rows, LANES), f32)
    block = 256
    for start in range(0, width, block):
        cols = slice(start, start + block)
        carried = dot(query, entering_ref[:, cols], ((1,), (0,)))
        scale = dot(factor, spread[:, cols], ((1,), (0,)))
        mixed = y_ref[:, cols] + carried * scale
        raw = mixed * silu(gate_ref[:, cols].astype(f32))
        for lane in range(0, block, LANES):
            piece = raw[:, lane : lane + LANES]
            squares = squares + piece * piece
        gated_ref[:, cols] = (raw * row_of(gain_ref, cols)).astype(bf16)
    total = jnp.sum(squares, axis=1, keepdims=True)
    squares_ref[...] = jnp.broadcast_to(total, (rows, LANES))
    high = total.astype(bf16)
    low = (total - high.astype(f32)).astype(bf16)
    lane = lax.broadcasted_iota(jnp.int32, (rows, LANES), 1)
    send_ref[:, width:] = jnp.where(
        lane < SPREAD,
        jnp.broadcast_to(high.astype(f32), (rows, LANES)),
        jnp.broadcast_to(low.astype(f32), (rows, LANES)),
    ).astype(bf16)
    first.wait()
    send_ref[:, :width] = dot(gated_ref[...], theirs_ref[...], ((1,), (0,))).astype(bf16)
    second.wait()


def own_kernel(gated_ref, weight_ref, own_ref):
    own_ref[...] = dot(gated_ref[...], weight_ref[...], ((1,), (0,)))


def finish_kernel(inner, own_ref, squares_ref, got_ref, out_ref):
    width = own_ref.shape[1]
    other = got_ref[:, width:].astype(f32)
    total = squares_ref[:, :1] + other[:, :1] + other[:, SPREAD : SPREAD + 1]
    scale = lax.rsqrt(total / inner + 1e-05)
    out_ref[...] = ((own_ref[...] + got_ref[:, :width].astype(f32)) * scale).astype(bf16)


VMEM = pl.BlockSpec(memory_space=pltpu.VMEM)
SMEM = pl.BlockSpec(memory_space=pltpu.SMEM)
HBM = pl.BlockSpec(memory_space=pltpu.HBM)


def call(kernel, specs, outs, flops, scratch=(), limit=40 << 20, out=VMEM):
    one = not isinstance(outs, (list, tuple))
    return pl.pallas_call(
        kernel,
        out_shape=outs,
        in_specs=specs,
        out_specs=out if one else [out] * len(outs),
        scratch_shapes=list(scratch),
        compiler_params=pltpu.CompilerParams(vmem_limit_bytes=limit),
        cost_estimate=pl.CostEstimate(flops=int(flops), bytes_accessed=1 << 20, transcendentals=0),
    )


WHOLE = 67043328
GATE_LIMIT = 44 << 20


def local(
    inner_input, gate_input, state_input, step_raw, conv_inner, conv_state,
    bias_inner, bias_state, step_bias, decay_log, skip_gain, norm_gain, out_weight,
):
    rows, width = inner_input.shape
    states = state_input.shape[1]
    half = states // 2
    devices = lax.axis_size("seq")
    halo = lax.ppermute(
        jnp.concatenate([inner_input[rows - 8 :], state_input[rows - 8 :]], axis=1),
        "seq",
        [(d, d + 1) for d in range(devices - 1)],
    )
    step_args = (step_raw, step_bias[None], decay_log[None])
    given = (
        halo, *step_args, conv_state, bias_state.reshape(-1, LANES), state_input,
        conv_inner, bias_inner.reshape(-1, LANES), inner_input,
    )
    shape = jax.ShapeDtypeStruct
    made = [((rows, width), bf16), ((rows, states), bf16), ((half, width + LANES), bf16)]
    x, bc, payload = call(
        functools.partial(update_kernel, len(given)),
        [HBM] * len(given),
        [shape(*m) for m in made],
        2e9,
        [pltpu.VMEM(v.shape, v.dtype) for v in given]
        + [pltpu.VMEM(*m) for m in made]
        + [
            pltpu.VMEM((rows + 8, width), f32),
            pltpu.VMEM((rows + 8, states), f32),
            pltpu.VMEM((2 * SPREAD, rows), f32),
            pltpu.SemaphoreType.DMA((len(given),)),
            pltpu.SemaphoreType.DMA((2 * (width // 256) + 2,)),
        ],
        WHOLE,
        HBM,
    )(*given)
    each = half // devices
    got = lax.all_to_all(
        payload.reshape(devices, each, width + LANES), "seq", split_axis=0, concat_axis=0, tiled=True
    )
    y = call(inside_kernel, [VMEM] * 5 + [SMEM], shape((rows, width), f32), 4e9)(
        x, bc, *step_args, skip_gain
    )
    before = call(
        functools.partial(prefix_kernel, devices), [VMEM], shape((half, width), bf16), 1e8
    )(got.reshape(half, width + LANES))
    entering = lax.all_to_all(
        before.reshape(devices, each, width), "seq", split_axis=0, concat_axis=0, tiled=True
    ).reshape(half, width)
    me = lax.axis_index("tp").astype(jnp.int32).reshape(1, 1)
    gated, squares, send, mine = call(
        gate_kernel,
        [SMEM] + [VMEM] * 8 + [HBM],
        [
            shape((rows, width), bf16), shape((rows, LANES), f32),
            shape((rows, width + LANES), bf16), shape((width, width), bf16),
        ],
        2e9,
        [
            pltpu.VMEM((2 * SPREAD, rows), f32),
            pltpu.VMEM((width, width), bf16),
            pltpu.SemaphoreType.DMA((2,)),
        ],
        GATE_LIMIT,
    )(me, entering, bc, y, *step_args, gate_input, norm_gain.reshape(-1, LANES), out_weight)
    pairs = lax.axis_size("tp")
    other = lax.ppermute(send, "tp", [(d, pairs - 1 - d) for d in range(pairs)])
    own = call(own_kernel, [VMEM, VMEM], shape((rows, width), f32), 2e9)(gated, mine)
    return call(
        functools.partial(finish_kernel, float(width * pairs)),
        [VMEM] * 3, shape((rows, width), bf16), 1e8,
    )(own, squares, other)


def solution(mesh):
    return jax.shard_map(
        local,
        mesh=mesh,
        in_specs=(
            P("seq", "tp"), P("seq", "tp"), P("seq", None), P("tp", "seq"), P(None, "tp"), P(),
            P("tp"), P(), P("tp"), P("tp"), P("tp"), P("tp"), P("tp", None),
        ),
        out_specs=P("seq", "tp"),
        check_vma=False,
    )
```

```python
import functools
import jax
import jax.numpy as jnp
from jax import lax
from jax.experimental import pallas as pl
from jax.experimental.pallas import tpu as pltpu
from jax.sharding import PartitionSpec as P

HEAD_DIM = 64
SPREAD = 64
LANES = 128
LOG2E = 1.4426950408889634
highest = lax.Precision.HIGHEST
f32 = jnp.float32
bf16 = jnp.bfloat16


def dot(a, b, contract, precision=None):
    return lax.dot_general(
        a, b, (contract, ((), ())), precision=precision, preferred_element_type=f32
    )


def silu(v):
    return v / (1.0 + jnp.exp(-v))


def spread_matrix(width):
    rows = lax.broadcasted_iota(jnp.int32, (2 * SPREAD, width), 0) & (SPREAD - 1)
    heads = lax.broadcasted_iota(jnp.int32, (2 * SPREAD, width), 1) >> (HEAD_DIM.bit_length() - 1)
    return jnp.where(rows == heads, 1.0, 0.0).astype(bf16)


def split_rows(ref, value):
    heads = value.shape[0]
    high = value.astype(bf16).astype(f32)
    ref[...] = jnp.zeros_like(ref)
    ref[0:heads, :] = high
    ref[SPREAD : SPREAD + heads, :] = value - high
    return ref[...].T.astype(bf16)


def as_column(row):
    count = row.shape[1]
    a = lax.broadcasted_iota(jnp.int32, (count, count), 0)
    b = lax.broadcasted_iota(jnp.int32, (count, count), 1)
    return jnp.sum(jnp.where(a == b, jnp.broadcast_to(row, (count, count)), 0.0), axis=1, keepdims=True)


def steps(raw_ref, step_bias_ref, decay_ref):
    v = raw_ref[...] + as_column(step_bias_ref[...])
    x = jnp.exp(-jnp.abs(v))
    series = x * (1.0 - x * (0.5 - x * (1.0 / 3.0 - x * 0.25)))
    size = jnp.maximum(v, 0.0) + jnp.where(x < 0.01, series, jnp.log(1.0 + x))
    return size, -jnp.exp(as_column(decay_ref[...])) * size


def lower(rows):
    t = lax.broadcasted_iota(jnp.int32, (rows, rows), 0)
    s = lax.broadcasted_iota(jnp.int32, (rows, rows), 1)
    return jnp.where(t >= s, 1.0, 0.0).astype(f32)


def row_of(ref, cols):
    first, last = cols.start // LANES, cols.stop // LANES
    return jnp.concatenate([ref[r : r + 1, :] for r in range(first, last)], axis=1)


def conv_block(scratch, taps_ref, bias_ref, cols, rows):
    taps = taps_ref.shape[0]
    first = 8 - (taps - 1)
    total = jnp.broadcast_to(row_of(bias_ref, cols), (rows, cols.stop - cols.start))
    for number in range(taps):
        total = total + taps_ref[number : number + 1, cols] * scratch[
            pl.ds(first + number, rows), cols
        ]
    return silu(total)


def update_kernel(count, *refs):
    sources, (x_out, bc_out, payload_out) = refs[:count], refs[count : count + 3]
    kept, rest = refs[count + 3 : 2 * count + 3], refs[2 * count + 3 :]
    (
        halo_ref, raw_ref, step_bias_ref, decay_ref, state_taps_ref, state_bias_ref, state_ref,
        taps_ref, bias_ref, inner_ref,
    ) = kept
    x_ref, bc_ref, payload_ref, pad, state_pad, parts, in_sems, out_sems = rest
    copies = [
        pltpu.make_async_copy(a, b, in_sems.at[i]) for i, (a, b) in enumerate(zip(sources, kept))
    ]
    for copy in copies:
        copy.start()
    for copy in copies[:-1]:
        copy.wait()
    rows, width = inner_ref.shape
    leaving = []

    def leave(source, target):
        copy = pltpu.make_async_copy(source, target, out_sems.at[len(leaving)])
        copy.start()
        leaving.append(copy)

    states = state_ref.shape[1]
    half = states // 2
    state_pad[0:8, :] = halo_ref[:, width:].astype(f32)
    state_pad[8:, :] = state_ref[...].astype(f32)
    bc_ref[...] = conv_block(state_pad, state_taps_ref, state_bias_ref, slice(0, states), rows).astype(bf16)
    leave(bc_ref, bc_out)
    keys = bc_ref[:, :half].astype(f32).T.astype(bf16)
    size, decay = steps(raw_ref, step_bias_ref, decay_ref)
    heads = raw_ref.shape[0]
    parts[...] = jnp.zeros_like(parts)
    parts[0:heads, :] = decay
    parts[SPREAD : SPREAD + heads, :] = decay
    total = jnp.exp(dot(jnp.ones((half, rows), f32), parts[...], ((1,), (1,)), highest))
    high = total.astype(bf16).astype(f32)
    lane = lax.broadcasted_iota(jnp.int32, (half, LANES), 1)
    payload_ref[:, width:] = jnp.where(lane < SPREAD, high, total - high).astype(bf16)
    cum = dot(decay, lower(rows), ((1,), (1,)), highest)
    weight = jnp.exp(cum[:, rows - 1 :] - cum) * size
    weight = split_rows(parts, weight)
    spread = spread_matrix(width)
    copies[-1].wait()
    pad[0:8, :] = halo_ref[:, :width].astype(f32)
    pad[8:, :] = inner_ref[...].astype(f32)
    last = slice(width, width + LANES)
    leave(payload_ref.at[:, last], payload_out.at[:, last])
    block = 256
    for start in range(0, width, block):
        cols = slice(start, start + block)
        value = conv_block(pad, taps_ref, bias_ref, cols, rows).astype(bf16)
        x_ref[:, cols] = value
        leave(x_ref.at[:, cols], x_out.at[:, cols])
        scale = dot(weight, spread[:, cols], ((1,), (0,)))
        scaled = (value.astype(f32) * scale).astype(bf16)
        payload_ref[:, cols] = dot(keys, scaled, ((1,), (0,))).astype(bf16)
        leave(payload_ref.at[:, cols], payload_out.at[:, cols])
    for copy in leaving:
        copy.wait()


def inside_kernel(x_ref, bc_ref, raw_ref, step_bias_ref, decay_ref, skip_ref, y_ref):
    rows = x_ref.shape[0]
    half = bc_ref.shape[1] // 2
    heads = raw_ref.shape[0]
    size, decay = steps(raw_ref, step_bias_ref, decay_ref)
    tri = lower(rows)
    cum = dot(decay, tri, ((1,), (1,)), highest) * LOG2E
    col = dot(tri, decay, ((1,), (1,)), highest) * LOG2E
    row = cum - jnp.log(size) * LOG2E
    mid = rows // 2
    scores = dot(bc_ref[:, half:], bc_ref[:, :half], ((1,), (1,)))
    causal = tri[:mid, :mid] > 0.5
    top = jnp.where(causal, scores[:mid, :mid], 0.0)
    low_left = scores[mid:, :mid]
    low_right = jnp.where(causal, scores[mid:, mid:], 0.0)
    for h in range(heads):
        cols = slice(h * HEAD_DIM, (h + 1) * HEAD_DIM)
        x = x_ref[:, cols]
        c0, c1 = col[:mid, h : h + 1], col[mid:, h : h + 1]
        r0, r1 = row[h : h + 1, :mid], row[h : h + 1, mid:]
        w0 = (top * jnp.exp2(jnp.minimum(c0 - r0, 100.0))).astype(bf16)
        w1 = (low_left * jnp.exp2(c1 - r0)).astype(bf16)
        w2 = (low_right * jnp.exp2(jnp.minimum(c1 - r1, 100.0))).astype(bf16)
        gain = skip_ref[h]
        y_ref[:mid, cols] = dot(w0, x[:mid], ((1,), (0,))) + gain * x[:mid].astype(f32)
        y_ref[mid:, cols] = (
            dot(w1, x[:mid], ((1,), (0,))) + dot(w2, x[mid:], ((1,), (0,)))
            + gain * x[mid:].astype(f32)
        )


def prefix_kernel(devices, got_ref, out_ref):
    width = out_ref.shape[1]
    each = got_ref.shape[0] // devices
    spread = spread_matrix(width)
    decays = dot(got_ref[:, width:], spread, ((1,), (0,)))
    update = got_ref[:, :width].astype(f32)
    running = jnp.zeros((each, width), f32)
    found = []
    for d in range(devices):
        found.append(running)
        rows = slice(d * each, (d + 1) * each)
        if d < devices - 1:
            running = running * decays[rows] + update[rows]
    out_ref[...] = jnp.concatenate(found, axis=0).astype(bf16)


def gate_kernel(
    me_ref, entering_ref, bc_ref, y_ref, raw_ref, step_bias_ref, decay_ref,
    gate_ref, gain_ref, weight_ref, gated_ref, squares_ref, send_ref,
    parts, theirs_ref, sem,
):
    rows, width = y_ref.shape
    peer = pl.multiple_of((1 - me_ref[0, 0]) * width, LANES)
    first = pltpu.make_async_copy(weight_ref.at[:, pl.ds(peer, width)], theirs_ref, sem)
    first.start()
    half = bc_ref.shape[1] // 2
    _, decay = steps(raw_ref, step_bias_ref, decay_ref)
    cum = jnp.exp(dot(decay, lower(rows), ((1,), (1,)), highest))
    factor = split_rows(parts, cum)
    spread = spread_matrix(width)
    query = bc_ref[:, half:]
    squares = jnp.zeros((rows, LANES), f32)
    block = 256
    for start in range(0, width, block):
        cols = slice(start, start + block)
        carried = dot(query, entering_ref[:, cols], ((1,), (0,)))
        scale = dot(factor, spread[:, cols], ((1,), (0,)))
        mixed = y_ref[:, cols] + carried * scale
        raw = mixed * silu(gate_ref[:, cols].astype(f32))
        for lane in range(0, block, LANES):
            piece = raw[:, lane : lane + LANES]
            squares = squares + piece * piece
        gated_ref[:, cols] = (raw * row_of(gain_ref, cols)).astype(bf16)
    total = jnp.sum(squares, axis=1, keepdims=True)
    squares_ref[...] = jnp.broadcast_to(total, (rows, LANES))
    high = total.astype(bf16)
    low = (total - high.astype(f32)).astype(bf16)
    lane = lax.broadcasted_iota(jnp.int32, (rows, LANES), 1)
    send_ref[:, width:] = jnp.where(
        lane < SPREAD,
        jnp.broadcast_to(high.astype(f32), (rows, LANES)),
        jnp.broadcast_to(low.astype(f32), (rows, LANES)),
    ).astype(bf16)
    first.wait()
    send_ref[:, :width] = dot(gated_ref[...], theirs_ref[...], ((1,), (0,))).astype(bf16)


def own_kernel(me_ref, gated_ref, weight_ref, own_ref, mine_ref, sems):
    width = gated_ref.shape[1]
    mine = pl.multiple_of(me_ref[0, 0] * width, LANES)
    half = width // 2
    parts = [slice(0, half), slice(half, width)]
    copies = [
        pltpu.make_async_copy(
            weight_ref.at[rows, pl.ds(mine, width)], mine_ref.at[rows, :], sems.at[i]
        )
        for i, rows in enumerate(parts)
    ]
    for copy in copies:
        copy.start()
    copies[0].wait()
    own_ref[...] = dot(gated_ref[:, parts[0]], mine_ref[parts[0], :], ((1,), (0,)))
    copies[1].wait()
    own_ref[...] += dot(gated_ref[:, parts[1]], mine_ref[parts[1], :], ((1,), (0,)))


def finish_kernel(inner, own_ref, squares_ref, got_ref, out_ref, kept, sems):
    height, width = own_ref.shape
    step = height // 4
    copies = []
    for number in range(4):
        rows = slice(number * step, (number + 1) * step)
        other = got_ref[rows, width:].astype(f32)
        total = squares_ref[rows, :1] + other[:, :1] + other[:, SPREAD : SPREAD + 1]
        scale = lax.rsqrt(total / inner + 1e-05)
        kept[rows, :] = ((own_ref[rows, :] + got_ref[rows, :width].astype(f32)) * scale).astype(bf16)
        copy = pltpu.make_async_copy(kept.at[rows, :], out_ref.at[rows, :], sems.at[number])
        copy.start()
        copies.append(copy)
    for copy in copies:
        copy.wait()


VMEM = pl.BlockSpec(memory_space=pltpu.VMEM)
SMEM = pl.BlockSpec(memory_space=pltpu.SMEM)
HBM = pl.BlockSpec(memory_space=pltpu.HBM)


def call(kernel, specs, outs, flops, scratch=(), limit=40 << 20, out=VMEM):
    one = not isinstance(outs, (list, tuple))
    return pl.pallas_call(
        kernel,
        out_shape=outs,
        in_specs=specs,
        out_specs=out if one else [out] * len(outs),
        scratch_shapes=list(scratch),
        compiler_params=pltpu.CompilerParams(vmem_limit_bytes=limit),
        cost_estimate=pl.CostEstimate(flops=int(flops), bytes_accessed=1 << 20, transcendentals=0),
    )


WHOLE = 67043328
GATE_LIMIT = 44 << 20
OWN_LIMIT = 52 << 20


def local(
    inner_input, gate_input, state_input, step_raw, conv_inner, conv_state,
    bias_inner, bias_state, step_bias, decay_log, skip_gain, norm_gain, out_weight,
):
    rows, width = inner_input.shape
    states = state_input.shape[1]
    half = states // 2
    devices = lax.axis_size("seq")
    shape = jax.ShapeDtypeStruct
    edge = jnp.concatenate([inner_input[rows - 8 :], state_input[rows - 8 :]], axis=1)
    halo = lax.ppermute(edge, "seq", [(d, d + 1) for d in range(devices - 1)])
    step_args = (step_raw, step_bias[None], decay_log[None])
    given = (
        halo, *step_args, conv_state, bias_state.reshape(-1, LANES), state_input,
        conv_inner, bias_inner.reshape(-1, LANES), inner_input,
    )
    shape = jax.ShapeDtypeStruct
    made = [((rows, width), bf16), ((rows, states), bf16), ((half, width + LANES), bf16)]
    x, bc, payload = call(
        functools.partial(update_kernel, len(given)),
        [HBM] * len(given),
        [shape(*m) for m in made],
        2e9,
        [pltpu.VMEM(v.shape, v.dtype) for v in given]
        + [pltpu.VMEM(*m) for m in made]
        + [
            pltpu.VMEM((rows + 8, width), f32),
            pltpu.VMEM((rows + 8, states), f32),
            pltpu.VMEM((2 * SPREAD, rows), f32),
            pltpu.SemaphoreType.DMA((len(given),)),
            pltpu.SemaphoreType.DMA((2 * (width // 256) + 2,)),
        ],
        WHOLE,
        HBM,
    )(*given)
    each = half // devices
    got = lax.all_to_all(
        payload.reshape(devices, each, width + LANES), "seq", split_axis=0, concat_axis=0, tiled=True
    )
    y = call(inside_kernel, [VMEM] * 5 + [SMEM], shape((rows, width), f32), 4e9)(
        x, bc, *step_args, skip_gain
    )
    before = call(
        functools.partial(prefix_kernel, devices), [VMEM], shape((half, width), bf16), 1e8
    )(got.reshape(half, width + LANES))
    entering = lax.all_to_all(
        before.reshape(devices, each, width), "seq", split_axis=0, concat_axis=0, tiled=True
    ).reshape(half, width)
    me = lax.axis_index("tp").astype(jnp.int32).reshape(1, 1)
    gated, squares, send = call(
        gate_kernel,
        [SMEM] + [VMEM] * 8 + [HBM],
        [
            shape((rows, width), bf16), shape((rows, LANES), f32),
            shape((rows, width + LANES), bf16),
        ],
        2e9,
        [
            pltpu.VMEM((2 * SPREAD, rows), f32),
            pltpu.VMEM((width, width), bf16),
            pltpu.SemaphoreType.DMA,
        ],
        GATE_LIMIT,
    )(me, entering, bc, y, *step_args, gate_input, norm_gain.reshape(-1, LANES), out_weight)
    pairs = lax.axis_size("tp")
    other = lax.ppermute(send, "tp", [(d, pairs - 1 - d) for d in range(pairs)])
    own = call(
        own_kernel, [SMEM, VMEM, HBM], shape((rows, width), f32), 2e9,
        [pltpu.VMEM((width, width), bf16), pltpu.SemaphoreType.DMA((2,))], OWN_LIMIT,
    )(me, gated, out_weight)
    return call(
        functools.partial(finish_kernel, float(width * pairs)),
        [VMEM] * 3, shape((rows, width), bf16), 1e8,
        [pltpu.VMEM((rows, width), bf16), pltpu.SemaphoreType.DMA((4,))],
        out=HBM,
    )(own, squares, other)


def solution(mesh):
    return jax.shard_map(
        local,
        mesh=mesh,
        in_specs=(
            P("seq", "tp"), P("seq", "tp"), P("seq", None), P("tp", "seq"), P(None, "tp"), P(),
            P("tp"), P(), P("tp"), P("tp"), P("tp"), P("tp"), P("tp", None),
        ),
        out_specs=P("seq", "tp"),
        check_vma=False,
    )
```

```python
import functools
import jax
import jax.numpy as jnp
from jax import lax
from jax.experimental import pallas as pl
from jax.experimental.pallas import tpu as pltpu
from jax.sharding import PartitionSpec as P

HEAD_DIM = 64
SPREAD = 64
LANES = 128
LOG2E = 1.4426950408889634
highest = lax.Precision.HIGHEST
f32 = jnp.float32
bf16 = jnp.bfloat16


def dot(a, b, contract, precision=None):
    return lax.dot_general(
        a, b, (contract, ((), ())), precision=precision, preferred_element_type=f32
    )


def silu(v):
    return v / (1.0 + jnp.exp(-v))


def spread_matrix(width):
    rows = lax.broadcasted_iota(jnp.int32, (2 * SPREAD, width), 0) & (SPREAD - 1)
    heads = lax.broadcasted_iota(jnp.int32, (2 * SPREAD, width), 1) >> (HEAD_DIM.bit_length() - 1)
    return jnp.where(rows == heads, 1.0, 0.0).astype(bf16)


def split_rows(ref, value):
    heads = value.shape[0]
    high = value.astype(bf16).astype(f32)
    ref[...] = jnp.zeros_like(ref)
    ref[0:heads, :] = high
    ref[SPREAD : SPREAD + heads, :] = value - high
    return ref[...].T.astype(bf16)


def as_column(row):
    count = row.shape[1]
    a = lax.broadcasted_iota(jnp.int32, (count, count), 0)
    b = lax.broadcasted_iota(jnp.int32, (count, count), 1)
    return jnp.sum(jnp.where(a == b, jnp.broadcast_to(row, (count, count)), 0.0), axis=1, keepdims=True)


def steps(raw_ref, step_bias_ref, decay_ref):
    v = raw_ref[...] + as_column(step_bias_ref[...])
    x = jnp.exp(-jnp.abs(v))
    series = x * (1.0 - x * (0.5 - x * (1.0 / 3.0 - x * 0.25)))
    size = jnp.maximum(v, 0.0) + jnp.where(x < 0.01, series, jnp.log(1.0 + x))
    return size, -jnp.exp(as_column(decay_ref[...])) * size


def lower(rows):
    t = lax.broadcasted_iota(jnp.int32, (rows, rows), 0)
    s = lax.broadcasted_iota(jnp.int32, (rows, rows), 1)
    return jnp.where(t >= s, 1.0, 0.0).astype(f32)


def row_of(ref, cols):
    first, last = cols.start // LANES, cols.stop // LANES
    return jnp.concatenate([ref[r : r + 1, :] for r in range(first, last)], axis=1)


def conv_block(scratch, taps_ref, bias_ref, cols, rows):
    taps = taps_ref.shape[0]
    first = 8 - (taps - 1)
    total = jnp.broadcast_to(row_of(bias_ref, cols), (rows, cols.stop - cols.start))
    for number in range(taps):
        total = total + taps_ref[number : number + 1, cols] * scratch[
            pl.ds(first + number, rows), cols
        ]
    return silu(total)


def update_kernel(count, *refs):
    sources, (x_out, bc_out, payload_out) = refs[:count], refs[count : count + 3]
    kept, rest = refs[count + 3 : 2 * count + 3], refs[2 * count + 3 :]
    (
        halo_ref, raw_ref, step_bias_ref, decay_ref, state_taps_ref, state_bias_ref, state_ref,
        taps_ref, bias_ref, inner_ref,
    ) = kept
    x_ref, bc_ref, payload_ref, pad, state_pad, parts, in_sems, out_sems = rest
    copies = [
        pltpu.make_async_copy(a, b, in_sems.at[i]) for i, (a, b) in enumerate(zip(sources, kept))
    ]
    for copy in copies:
        copy.start()
    for copy in copies[:-1]:
        copy.wait()
    rows, width = inner_ref.shape
    leaving = []

    def leave(source, target):
        copy = pltpu.make_async_copy(source, target, out_sems.at[len(leaving)])
        copy.start()
        leaving.append(copy)

    states = state_ref.shape[1]
    half = states // 2
    state_pad[0:8, :] = halo_ref[:, width:].astype(f32)
    state_pad[8:, :] = state_ref[...].astype(f32)
    bc_ref[...] = conv_block(state_pad, state_taps_ref, state_bias_ref, slice(0, states), rows).astype(bf16)
    leave(bc_ref, bc_out)
    keys = bc_ref[:, :half].astype(f32).T.astype(bf16)
    size, decay = steps(raw_ref, step_bias_ref, decay_ref)
    heads = raw_ref.shape[0]
    parts[...] = jnp.zeros_like(parts)
    parts[0:heads, :] = decay
    parts[SPREAD : SPREAD + heads, :] = decay
    total = jnp.exp(dot(jnp.ones((half, rows), f32), parts[...], ((1,), (1,)), highest))
    high = total.astype(bf16).astype(f32)
    lane = lax.broadcasted_iota(jnp.int32, (half, LANES), 1)
    payload_ref[:, width:] = jnp.where(lane < SPREAD, high, total - high).astype(bf16)
    cum = dot(decay, lower(rows), ((1,), (1,)), highest)
    weight = jnp.exp(cum[:, rows - 1 :] - cum) * size
    weight = split_rows(parts, weight)
    spread = spread_matrix(width)
    copies[-1].wait()
    pad[0:8, :] = halo_ref[:, :width].astype(f32)
    pad[8:, :] = inner_ref[...].astype(f32)
    last = slice(width, width + LANES)
    leave(payload_ref.at[:, last], payload_out.at[:, last])
    block = 256
    for start in range(0, width, block):
        cols = slice(start, start + block)
        value = conv_block(pad, taps_ref, bias_ref, cols, rows).astype(bf16)
        x_ref[:, cols] = value
        leave(x_ref.at[:, cols], x_out.at[:, cols])
        scale = dot(weight, spread[:, cols], ((1,), (0,)))
        scaled = (value.astype(f32) * scale).astype(bf16)
        payload_ref[:, cols] = dot(keys, scaled, ((1,), (0,))).astype(bf16)
        leave(payload_ref.at[:, cols], payload_out.at[:, cols])
    for copy in leaving:
        copy.wait()


def inside_kernel(x_ref, bc_ref, raw_ref, step_bias_ref, decay_ref, skip_ref, y_ref):
    rows = x_ref.shape[0]
    half = bc_ref.shape[1] // 2
    heads = raw_ref.shape[0]
    size, decay = steps(raw_ref, step_bias_ref, decay_ref)
    tri = lower(rows)
    cum = dot(decay, tri, ((1,), (1,)), highest) * LOG2E
    col = dot(tri, decay, ((1,), (1,)), highest) * LOG2E
    row = cum - jnp.log(size) * LOG2E
    mid = rows // 2
    scores = dot(bc_ref[:, half:], bc_ref[:, :half], ((1,), (1,)))
    causal = tri[:mid, :mid] > 0.5
    top = jnp.where(causal, scores[:mid, :mid], 0.0)
    low_left = scores[mid:, :mid]
    low_right = jnp.where(causal, scores[mid:, mid:], 0.0)
    for h in range(heads):
        cols = slice(h * HEAD_DIM, (h + 1) * HEAD_DIM)
        x = x_ref[:, cols]
        c0, c1 = col[:mid, h : h + 1], col[mid:, h : h + 1]
        r0, r1 = row[h : h + 1, :mid], row[h : h + 1, mid:]
        w0 = (top * jnp.exp2(jnp.minimum(c0 - r0, 100.0))).astype(bf16)
        w1 = (low_left * jnp.exp2(c1 - r0)).astype(bf16)
        w2 = (low_right * jnp.exp2(jnp.minimum(c1 - r1, 100.0))).astype(bf16)
        gain = skip_ref[h]
        y_ref[:mid, cols] = dot(w0, x[:mid], ((1,), (0,))) + gain * x[:mid].astype(f32)
        y_ref[mid:, cols] = (
            dot(w1, x[:mid], ((1,), (0,))) + dot(w2, x[mid:], ((1,), (0,)))
            + gain * x[mid:].astype(f32)
        )


def prefix_kernel(devices, got_ref, out_ref):
    width = out_ref.shape[1]
    each = got_ref.shape[0] // devices
    spread = spread_matrix(width)
    decays = dot(got_ref[:, width:], spread, ((1,), (0,)))
    update = got_ref[:, :width].astype(f32)
    running = jnp.zeros((each, width), f32)
    found = []
    for d in range(devices):
        found.append(running)
        rows = slice(d * each, (d + 1) * each)
        if d < devices - 1:
            running = running * decays[rows] + update[rows]
    out_ref[...] = jnp.concatenate(found, axis=0).astype(bf16)


def gate_kernel(
    me_ref, entering_ref, bc_ref, y_ref, raw_ref, step_bias_ref, decay_ref,
    gate_ref, gain_ref, weight_ref, gated_ref, squares_ref, send_ref,
    parts, theirs_ref, sem,
):
    rows, width = y_ref.shape
    peer = pl.multiple_of((1 - me_ref[0, 0]) * width, LANES)
    step = width // 8
    pieces = [slice(i * step, (i + 1) * step) for i in range(8)]
    copies = [
        pltpu.make_async_copy(weight_ref.at[p, pl.ds(peer, width)], theirs_ref.at[p, :], sem.at[i])
        for i, p in enumerate(pieces)
    ]
    for copy in copies:
        copy.start()
    half = bc_ref.shape[1] // 2
    _, decay = steps(raw_ref, step_bias_ref, decay_ref)
    cum = jnp.exp(dot(decay, lower(rows), ((1,), (1,)), highest))
    factor = split_rows(parts, cum)
    spread = spread_matrix(width)
    query = bc_ref[:, half:]
    squares = jnp.zeros((rows, LANES), f32)
    block = 256
    for start in range(0, width, block):
        cols = slice(start, start + block)
        carried = dot(query, entering_ref[:, cols], ((1,), (0,)))
        scale = dot(factor, spread[:, cols], ((1,), (0,)))
        mixed = y_ref[:, cols] + carried * scale
        raw = mixed * silu(gate_ref[:, cols].astype(f32))
        for lane in range(0, block, LANES):
            piece = raw[:, lane : lane + LANES]
            squares = squares + piece * piece
        gated_ref[:, cols] = (raw * row_of(gain_ref, cols)).astype(bf16)
    total = jnp.sum(squares, axis=1, keepdims=True)
    squares_ref[...] = jnp.broadcast_to(total, (rows, LANES))
    high = total.astype(bf16)
    low = (total - high.astype(f32)).astype(bf16)
    lane = lax.broadcasted_iota(jnp.int32, (rows, LANES), 1)
    send_ref[:, width:] = jnp.where(
        lane < SPREAD,
        jnp.broadcast_to(high.astype(f32), (rows, LANES)),
        jnp.broadcast_to(low.astype(f32), (rows, LANES)),
    ).astype(bf16)
    for copy in copies:
        copy.wait()
    send_ref[:, :width] = dot(gated_ref[...], theirs_ref[...], ((1,), (0,))).astype(bf16)


def own_kernel(me_ref, gated_ref, weight_ref, own_ref, mine_ref, sems):
    width = gated_ref.shape[1]
    mine = pl.multiple_of(me_ref[0, 0] * width, LANES)
    half = width // 2
    step = width // 8
    parts = [slice(i * step, (i + 1) * step) for i in range(8)]
    copies = [
        pltpu.make_async_copy(
            weight_ref.at[rows, pl.ds(mine, width)], mine_ref.at[rows, :], sems.at[i]
        )
        for i, rows in enumerate(parts)
    ]
    for copy in copies:
        copy.start()
    for copy in copies[:4]:
        copy.wait()
    own_ref[...] = dot(gated_ref[:, :half], mine_ref[:half, :], ((1,), (0,)))
    for copy in copies[4:]:
        copy.wait()
    own_ref[...] += dot(gated_ref[:, half:], mine_ref[half:, :], ((1,), (0,)))


def finish_kernel(inner, own_ref, squares_ref, got_ref, out_ref, kept, sems):
    height, width = own_ref.shape
    step = height // 4
    copies = []
    for number in range(4):
        rows = slice(number * step, (number + 1) * step)
        other = got_ref[rows, width:].astype(f32)
        total = squares_ref[rows, :1] + other[:, :1] + other[:, SPREAD : SPREAD + 1]
        scale = lax.rsqrt(total / inner + 1e-05)
        kept[rows, :] = ((own_ref[rows, :] + got_ref[rows, :width].astype(f32)) * scale).astype(bf16)
        copy = pltpu.make_async_copy(kept.at[rows, :], out_ref.at[rows, :], sems.at[number])
        copy.start()
        copies.append(copy)
    for copy in copies:
        copy.wait()


VMEM = pl.BlockSpec(memory_space=pltpu.VMEM)
SMEM = pl.BlockSpec(memory_space=pltpu.SMEM)
HBM = pl.BlockSpec(memory_space=pltpu.HBM)


def call(kernel, specs, outs, flops, scratch=(), limit=40 << 20, out=VMEM):
    one = not isinstance(outs, (list, tuple))
    return pl.pallas_call(
        kernel,
        out_shape=outs,
        in_specs=specs,
        out_specs=out if one else [out] * len(outs),
        scratch_shapes=list(scratch),
        compiler_params=pltpu.CompilerParams(vmem_limit_bytes=limit),
        cost_estimate=pl.CostEstimate(flops=int(flops), bytes_accessed=1 << 20, transcendentals=0),
    )


WHOLE = 67043328
GATE_LIMIT = 44 << 20
OWN_LIMIT = 52 << 20


def local(
    inner_input, gate_input, state_input, step_raw, conv_inner, conv_state,
    bias_inner, bias_state, step_bias, decay_log, skip_gain, norm_gain, out_weight,
):
    rows, width = inner_input.shape
    states = state_input.shape[1]
    half = states // 2
    devices = lax.axis_size("seq")
    shape = jax.ShapeDtypeStruct
    edge = jnp.concatenate([inner_input[rows - 8 :], state_input[rows - 8 :]], axis=1)
    halo = lax.ppermute(edge, "seq", [(d, d + 1) for d in range(devices - 1)])
    step_args = (step_raw, step_bias[None], decay_log[None])
    given = (
        halo, *step_args, conv_state, bias_state.reshape(-1, LANES), state_input,
        conv_inner, bias_inner.reshape(-1, LANES), inner_input,
    )
    shape = jax.ShapeDtypeStruct
    made = [((rows, width), bf16), ((rows, states), bf16), ((half, width + LANES), bf16)]
    x, bc, payload = call(
        functools.partial(update_kernel, len(given)),
        [HBM] * len(given),
        [shape(*m) for m in made],
        2e9,
        [pltpu.VMEM(v.shape, v.dtype) for v in given]
        + [pltpu.VMEM(*m) for m in made]
        + [
            pltpu.VMEM((rows + 8, width), f32),
            pltpu.VMEM((rows + 8, states), f32),
            pltpu.VMEM((2 * SPREAD, rows), f32),
            pltpu.SemaphoreType.DMA((len(given),)),
            pltpu.SemaphoreType.DMA((2 * (width // 256) + 2,)),
        ],
        WHOLE,
        HBM,
    )(*given)
    each = half // devices
    got = lax.all_to_all(
        payload.reshape(devices, each, width + LANES), "seq", split_axis=0, concat_axis=0, tiled=True
    )
    y = call(inside_kernel, [VMEM] * 5 + [SMEM], shape((rows, width), f32), 4e9)(
        x, bc, *step_args, skip_gain
    )
    before = call(
        functools.partial(prefix_kernel, devices), [VMEM], shape((half, width), bf16), 1e8
    )(got.reshape(half, width + LANES))
    entering = lax.all_to_all(
        before.reshape(devices, each, width), "seq", split_axis=0, concat_axis=0, tiled=True
    ).reshape(half, width)
    me = lax.axis_index("tp").astype(jnp.int32).reshape(1, 1)
    gated, squares, send = call(
        gate_kernel,
        [SMEM] + [VMEM] * 8 + [HBM],
        [
            shape((rows, width), bf16), shape((rows, LANES), f32),
            shape((rows, width + LANES), bf16),
        ],
        2e9,
        [
            pltpu.VMEM((2 * SPREAD, rows), f32),
            pltpu.VMEM((width, width), bf16),
            pltpu.SemaphoreType.DMA((8,)),
        ],
        GATE_LIMIT,
    )(me, entering, bc, y, *step_args, gate_input, norm_gain.reshape(-1, LANES), out_weight)
    pairs = lax.axis_size("tp")
    other = lax.ppermute(send, "tp", [(d, pairs - 1 - d) for d in range(pairs)])
    own = call(
        own_kernel, [SMEM, VMEM, HBM], shape((rows, width), f32), 2e9,
        [pltpu.VMEM((width, width), bf16), pltpu.SemaphoreType.DMA((8,))], OWN_LIMIT,
    )(me, gated, out_weight)
    return call(
        functools.partial(finish_kernel, float(width * pairs)),
        [VMEM] * 3, shape((rows, width), bf16), 1e8,
        [pltpu.VMEM((rows, width), bf16), pltpu.SemaphoreType.DMA((4,))],
        out=HBM,
    )(own, squares, other)


def solution(mesh):
    return jax.shard_map(
        local,
        mesh=mesh,
        in_specs=(
            P("seq", "tp"), P("seq", "tp"), P("seq", None), P("tp", "seq"), P(None, "tp"), P(),
            P("tp"), P(), P("tp"), P("tp"), P("tp"), P("tp"), P("tp", None),
        ),
        out_specs=P("seq", "tp"),
        check_vma=False,
    )
```
